32 devices in a mesh: fsdp: 16 (over z, y, x), seq: 2 (over core).
Axes of the slice: x: 2, y: 2, z: 4, core: 2. Of those that a mesh axis runs over, the one named last changes fastest.
Arguments:
- tokens: bfloat16 [16, 768, 2048], P('fsdp', 'seq'), may hold values from -6 to 6
- segment_ids: int32 [16, 768], P('fsdp'), may hold values from 0 to 2, never falling along the last dimension, each value on 1 to 384 neighbouring positions
- piece_starts: int32 [16], P('fsdp'), may hold values from 0 to 512
- kv_cotangent: bfloat16 [16, 768, 256], P('fsdp', 'seq'), may hold values from -6 to 6
- out_cotangent: bfloat16 [16, 768, 2048], P('fsdp', 'seq'), may hold values from -6 to 6
- attn_gain: bfloat16 [2048], P(('fsdp', 'seq')), may hold values from 0.5 to 1.5
- w_query: bfloat16 [2048, 2048], P(('fsdp', 'seq')), may hold values from -0.125 to 0.125
- w_key: bfloat16 [2048, 128], P(('fsdp', 'seq')), may hold values from -0.125 to 0.125
- w_value: bfloat16 [2048, 128], P(('fsdp', 'seq')), may hold values from -0.125 to 0.125
- output_weight: bfloat16 [2048, 2048], P(('fsdp', 'seq')), may hold values from -0.75 to 0.75
- ffn_gain: bfloat16 [2048], P(('fsdp', 'seq')), may hold values from 0.5 to 1.5
- w_gate: bfloat16 [2048, 5632], P(('fsdp', 'seq')), may hold values from -0.125 to 0.125
- w_up: bfloat16 [2048, 5632], P(('fsdp', 'seq')), may hold values from -0.125 to 0.125
- w_down: bfloat16 [2048, 5632], P(('fsdp', 'seq')), may hold values from -0.078125 to 0.078125
Outputs:
- layer_output: bfloat16 [16, 768, 2048], P('fsdp', 'seq')
- input_grad: bfloat16 [16, 768, 2048], P('fsdp', 'seq')
- attn_gain_grad: float32 [2048], P(('fsdp', 'seq'))
- query_grad: float32 [2048, 2048], P(('fsdp', 'seq'))
- key_grad: float32 [2048, 128], P(('fsdp', 'seq'))
- value_grad: float32 [2048, 128], P(('fsdp', 'seq'))
- w_out_grad: float32 [2048, 2048], P(('fsdp', 'seq'))
- ffn_gain_grad: float32 [2048], P(('fsdp', 'seq'))
- gate_grad: float32 [2048, 5632], P(('fsdp', 'seq'))
- up_grad: float32 [2048, 5632], P(('fsdp', 'seq'))
- down_grad: float32 [2048, 5632], P(('fsdp', 'seq'))
The draws below stay inside these ranges and needn't reach their ends.
Inputs may be any that keep to these rules, and one draw needn't show every extreme that they name: `segment_ids`: in each sequence the document numbers start at 0, never fall and take each of 0, 1, 2 for 1 to 384 positions; one document has exactly 384.
All inputs are finite; a program needn't handle non-finite values.
Results may differ from the reference program's by a relative error of at most 0.015.
Values may be sent and summed in bfloat16 or wider, within the bound.
A program may use at most 448 MiB of HBM per device.

```python
import math
import jax
import jax.numpy as jnp
import numpy as np
from jax import lax

MODEL_WIDTH = 2048
HEADS = 16
HEAD_DIM = 128
FF = 5632
PIECE = 256
SEQUENCE_LENGTH = 768
GROUPS = 16


def place_ends(values, own_key, least, top_value):
    index_at = [jax.random.randint(jax.random.fold_in(own_key, axis), (), 0, length) for axis, length in enumerate(values.shape)]
    main_axis = values.shape.index(max(values.shape))
    next_to = index_at[:main_axis] + [(index_at[main_axis] + 1) % values.shape[main_axis]] + index_at[main_axis + 1:]
    return values.at[tuple(index_at)].set(least).at[tuple(next_to)].set(top_value)


def shard_levels(own_key, extent, pieces, low, top_value):
    level, own = 1.0, jax.random.fold_in(own_key, 6)
    for position, shards_of in pieces:
        steps = jnp.exp(jax.random.uniform(jax.random.fold_in(own, position), (shards_of,), jnp.float32, low / len(pieces), top_value / len(pieces)))
        level = level * jnp.repeat(steps, extent[position] // shards_of).reshape([-1 if axis == position else 1 for axis in range(len(extent))])
    return level


def length_profile(number_of, total, limit, lean):
    loads = [(1 << 20) // math.isqrt(grade ** lean) + 1 for grade in range(2, number_of + 1)]
    spare, counts = total - limit - (number_of - 1), [1] * (number_of - 1)
    while spare > 0:
        movable = [i for i in range(number_of - 1) if counts[i] < limit]
        whole, budget = sum([loads[i] for i in movable]), spare
        for i in movable:
            addition = min(limit - counts[i], max(1, budget * loads[i] // whole), spare)
            counts[i] = counts[i] + addition
            spare = spare - addition
    return np.array([limit] + counts)


def ragged_sizes(stream_key, count, total, limit, skew):
    if count == 2:
        one = jax.random.randint(stream_key, (), max(1, total - limit), min(limit, total - 1) + 1)
        return jnp.stack([one, total - one])
    lengths = jnp.asarray(length_profile(count, total, limit, skew), jnp.int32)
    twos = (count - 1) // 2
    giver, taker = lengths[1:1 + 2 * twos:2], lengths[2:2 + 2 * twos:2]
    margin = jnp.minimum(giver - 1, limit - taker)
    passed = jax.random.randint(jax.random.fold_in(stream_key, 1), (twos,), 0, 1 << 20) % (margin + 1)
    lengths = lengths.at[1:1 + 2 * twos:2].set(giver - passed).at[2:2 + 2 * twos:2].set(taker + passed)
    return lengths[jax.random.permutation(jax.random.fold_in(stream_key, 2), count)]


def scatter_about(own_key, extent, scale, limit, cuts=(), kind=jnp.bfloat16):
    entries = scale * jax.random.normal(own_key, extent, jnp.float32)
    if cuts:
        entries = entries * shard_levels(own_key, extent, cuts, -0.22, 0.18)
    return jnp.clip(entries, -limit, limit).astype(kind)


def setup_inputs(seed: int = 0) -> dict:
    seeds = jax.random.split(jax.random.key(seed), 15)
    return {
        "tokens": scatter_about(seeds[0], (GROUPS, SEQUENCE_LENGTH, MODEL_WIDTH), 1.0, 6.0, ((0, 16), (1, 2))),
        "segment_ids": jax.vmap(lambda own: jnp.searchsorted(jnp.cumsum(ragged_sizes(own, 3, SEQUENCE_LENGTH, SEQUENCE_LENGTH // 2, 0)), jnp.arange(SEQUENCE_LENGTH), side="right"))(jax.random.split(seeds[1], GROUPS)).reshape((GROUPS, SEQUENCE_LENGTH)).astype(jnp.int32),
        "piece_starts": place_ends(jax.random.randint(seeds[2], (GROUPS,), 0, SEQUENCE_LENGTH - PIECE + 1), jax.random.fold_in(seeds[2], 1), 0, SEQUENCE_LENGTH - PIECE).astype(jnp.int32),
        "kv_cotangent": scatter_about(seeds[3], (GROUPS, SEQUENCE_LENGTH, 2 * HEAD_DIM), 0.5, 6.0, ((0, 16), (1, 2))),
        "out_cotangent": scatter_about(seeds[4], (GROUPS, SEQUENCE_LENGTH, MODEL_WIDTH), 1.0, 6.0, ((0, 16), (1, 2))),
        "attn_gain": jnp.clip(1.0 + 0.1 * jax.random.normal(seeds[5], (MODEL_WIDTH,), jnp.float32), 0.5, 1.5).astype(jnp.bfloat16),
        "w_query": scatter_about(seeds[6], (MODEL_WIDTH, MODEL_WIDTH), MODEL_WIDTH ** -0.5, 0.125, ((0, 32),)),
        "w_key": scatter_about(seeds[7], (MODEL_WIDTH, HEAD_DIM), MODEL_WIDTH ** -0.5, 0.125, ((0, 32),)),
        "w_value": scatter_about(seeds[8], (MODEL_WIDTH, HEAD_DIM), MODEL_WIDTH ** -0.5, 0.125, ((0, 32),)),
        "output_weight": scatter_about(seeds[9], (MODEL_WIDTH, MODEL_WIDTH), (MODEL_WIDTH // 32) ** -0.5, 0.75, ((0, 32),)),
        "ffn_gain": jnp.clip(1.0 + 0.1 * jax.random.normal(seeds[10], (MODEL_WIDTH,), jnp.float32), 0.5, 1.5).astype(jnp.bfloat16),
        "w_gate": scatter_about(seeds[11], (MODEL_WIDTH, FF), MODEL_WIDTH ** -0.5, 0.125, ((0, 32),)),
        "w_up": scatter_about(seeds[12], (MODEL_WIDTH, FF), MODEL_WIDTH ** -0.5, 0.125, ((0, 32),)),
        "w_down": scatter_about(seeds[13], (MODEL_WIDTH, FF), FF ** -0.5, 0.078125, ((0, 32),)),
    }


@jax.custom_vjp
def low(v):
    return lax.optimization_barrier(v.astype(jnp.bfloat16)).astype(jnp.float32)

@jax.custom_vjp
def low_back(v):
    return v

def low_keep(v):
    return (low(v), None)

def low_pass(kept, grad):
    return (grad,)

def back_keep(v):
    return (v, None)

def back_low(kept, grad):
    return (low(grad),)
low.defvjp(low_keep, low_pass)
low_back.defvjp(back_keep, back_low)
highest_precision = lax.Precision.HIGHEST
norm_epsilon = 1e-05
rope_base = 10000.0
masked_score = -1e+30

def rope_tables(positions, breadth):
    halfway = breadth // 2
    ladder = jnp.arange(halfway, dtype=jnp.float32) * (2.0 / breadth)
    frequency = rope_base ** (-ladder)
    angles = positions.astype(jnp.float32)[:, None] * frequency[None, :]
    angles = jnp.concatenate([angles, angles], axis=1)
    return (jnp.cos(angles), jnp.sin(angles))

def rotate(vectors, cosine, sine_tab):
    halfway = vectors.shape[-1] // 2
    turned = jnp.concatenate([-vectors[..., halfway:], vectors[..., :halfway]], axis=-1)
    return vectors * cosine + turned * sine_tab

def rms_normed(value_rows):
    return value_rows * lax.rsqrt(lax.optimization_barrier(jnp.mean(value_rows * value_rows, axis=-1, keepdims=True)) + norm_epsilon)

def layer_fwd(tok_rows, seg_rows, start_rows, attn_gain, w_query, w_key, w_value, output_weight, ffn_gain, w_gate, w_up, w_down):
    sequence_count = tok_rows.shape[0]
    positions = jnp.arange(SEQUENCE_LENGTH, dtype=jnp.int32)
    cosine, sine_tab = rope_tables(positions, HEAD_DIM)
    normed = rms_normed(tok_rows)
    hidden = low(normed * attn_gain)
    query_pre = low_back(jnp.einsum('bld,de->ble', hidden, w_query, precision=highest_precision))
    key_pre = low_back(jnp.einsum('bld,de->ble', hidden, w_key, precision=highest_precision))
    value_rows = low(low_back(jnp.einsum('bld,de->ble', hidden, w_value, precision=highest_precision)))
    query_heads = query_pre.reshape(sequence_count, SEQUENCE_LENGTH, HEADS, HEAD_DIM)
    query_rows_all = low(rotate(query_heads, cosine[:, None, :], sine_tab[:, None, :]) * HEAD_DIM ** (-0.5))
    rotated_keys = low(rotate(key_pre, cosine, sine_tab))
    same_doc = seg_rows[:, :, None] == seg_rows[:, None, :]
    causal = positions[:, None] >= positions[None, :]
    inside = (positions[None, :] >= start_rows[:, None]) & (positions[None, :] < start_rows[:, None] + PIECE)
    visible = same_doc & (causal[None] | inside[:, :, None] & inside[:, None, :])
    attention_scores = low_back(jnp.einsum('loas,lps->laop', query_rows_all, rotated_keys, precision=highest_precision))
    attention_scores = jnp.where(visible[:, None], attention_scores, masked_score)
    attention_probs = low(jax.nn.softmax(attention_scores, axis=-1))
    attention_mixed = jnp.einsum('cwej,cjm->cewm', attention_probs, value_rows, precision=highest_precision).reshape(sequence_count, SEQUENCE_LENGTH, MODEL_WIDTH)
    attention_mixed = low(low_back(attention_mixed))
    branch_output = low_back(jnp.einsum('ijz,xz->ijx', attention_mixed, output_weight, precision=highest_precision))
    residual = tok_rows + branch_output
    hidden_two = low(rms_normed(residual) * ffn_gain)
    gate_pre = low_back(jnp.einsum('bld,df->blf', hidden_two, w_gate, precision=highest_precision))
    up_pre = low_back(jnp.einsum('bld,df->blf', hidden_two, w_up, precision=highest_precision))
    act_rows = low(jax.nn.silu(gate_pre) * up_pre)
    ffn_branch = low_back(jnp.einsum('blf,df->bld', act_rows, w_down, precision=highest_precision))
    shared = jnp.concatenate([rotated_keys, value_rows], axis=-1)
    return (residual + ffn_branch, shared)

def reference(tokens, segment_ids, piece_starts, kv_cotangent, out_cotangent, attn_gain, w_query, w_key, w_value, output_weight, ffn_gain, w_gate, w_up, w_down):
    total_seq = GROUPS
    per_block = math.gcd(total_seq, max(1, 3072 // SEQUENCE_LENGTH))
    blocks_n = total_seq // per_block
    weights = tuple((weight.astype(jnp.float32) for weight in (attn_gain, w_query, w_key, w_value, output_weight, ffn_gain, w_gate, w_up, w_down)))
    tok_blocks = tokens.astype(jnp.float32).reshape(blocks_n, per_block, SEQUENCE_LENGTH, MODEL_WIDTH)
    seg_blocks = segment_ids.reshape(blocks_n, per_block, SEQUENCE_LENGTH).astype(jnp.int32)
    start_blocks = piece_starts.reshape(blocks_n, per_block).astype(jnp.int32)

    def run_blocks(weight_set, tok_all):

        def scan_step(carried, inputs):
            tok_rows, seg_rows, start_rows = inputs
            return (carried, layer_fwd(tok_rows, seg_rows, start_rows, *weight_set))
        unused, results = lax.scan(jax.checkpoint(scan_step), jnp.zeros((), jnp.float32), (tok_all, seg_blocks, start_blocks))
        return results
    (outs_all, shared_all), pullback = jax.vjp(run_blocks, weights, tok_blocks)
    cot_out = out_cotangent.astype(jnp.float32).reshape(blocks_n, per_block, SEQUENCE_LENGTH, MODEL_WIDTH)
    cot_kv = kv_cotangent.astype(jnp.float32).reshape(blocks_n, per_block, SEQUENCE_LENGTH, 2 * HEAD_DIM)
    weight_grads, token_grads = pullback((cot_out, cot_kv))
    layer_output = outs_all.reshape(GROUPS, SEQUENCE_LENGTH, MODEL_WIDTH).astype(jnp.bfloat16)
    input_grad = token_grads.reshape(GROUPS, SEQUENCE_LENGTH, MODEL_WIDTH).astype(jnp.bfloat16)
    return (layer_output, input_grad, weight_grads[0], weight_grads[1], weight_grads[2], weight_grads[3], weight_grads[4], weight_grads[5], weight_grads[6], weight_grads[7], weight_grads[8])
```

```python
import jax
import jax.numpy as jnp
from jax import lax
from jax.sharding import PartitionSpec as P

PIECE = 256

norm_epsilon = 1e-05
rope_base = 10000.0
masked_score = -1e30

bf16 = jnp.bfloat16
f32 = jnp.float32


def rope_tables(positions, breadth):
    halfway = breadth // 2
    ladder = jnp.arange(halfway, dtype=f32) * (2.0 / breadth)
    frequency = rope_base ** (-ladder)
    angles = positions.astype(f32)[:, None] * frequency[None, :]
    angles = jnp.concatenate([angles, angles], axis=1)
    return (jnp.cos(angles), jnp.sin(angles))


def rotate(vectors, cosine, sine_tab):
    halfway = vectors.shape[-1] // 2
    turned = jnp.concatenate([-vectors[..., halfway:], vectors[..., :halfway]], axis=-1)
    return vectors * cosine + turned * sine_tab


def rms_scale(value_rows):
    return lax.rsqrt(jnp.mean(value_rows * value_rows, axis=-1) + norm_epsilon)


def norm_back(dnormed, normed, scales):
    inner_sum = jnp.mean(dnormed * normed, axis=-1, keepdims=True)
    return scales[:, None] * (dnormed - normed * inner_sum)


def dot_nn(a, b):
    return lax.dot_general(a, b, (((1,), (0,)), ((), ())), preferred_element_type=f32)


def dot_nt(a, b):
    return lax.dot_general(a, b, (((1,), (1,)), ((), ())), preferred_element_type=f32)


def dot_tn(a, b):
    return lax.dot_general(a, b, (((0,), (0,)), ((), ())), preferred_element_type=f32)


def halves(v):
    middle = v.shape[0] // 2
    return v[:middle], v[middle:]


def swap_rows(v):
    low, high = halves(v)
    return jnp.concatenate([high, low], axis=0)


class Cube:
    def __init__(self, chips, width):
        self.chips = chips
        self.bits = chips.bit_length() - 1
        self.width = width
        self.block = width // chips
        self.mine = lax.axis_index("fsdp")
        self.core = lax.axis_index("seq")

    def order(self, first):
        return tuple(b for b in first if b < self.bits) + tuple(
            b for b in range(self.bits) if b not in first
        )

    def rel(self, order, position):
        return sum(((position >> (self.bits - 1 - i)) & 1) << b for i, b in enumerate(order))

    def place(self, order, rel):
        return sum(((rel >> b) & 1) << (self.bits - 1 - i) for i, b in enumerate(order))

    def cross(self, v, bit):
        return lax.ppermute(v, "fsdp", [(i, i ^ (1 << bit)) for i in range(self.chips)])

    def other_core(self, v):
        return lax.ppermute(v, "seq", [(0, 1), (1, 0)])

    def pick(self, if_zero, if_one):
        return jnp.where(self.core == 0, if_zero, if_one)

    def to_space(self, v, order):
        starts = [(self.rel(order, p) ^ self.mine) * self.block for p in range(self.chips)]
        return jnp.concatenate(
            [lax.dynamic_slice_in_dim(v, s, self.block, axis=1) for s in starts], axis=1
        )

    def from_space(self, v, order):
        starts = [self.place(order, j ^ self.mine) * self.block for j in range(self.chips)]
        return jnp.concatenate(
            [lax.dynamic_slice_in_dim(v, s, self.block, axis=1) for s in starts], axis=1
        )

    def respace(self, v, source, target):
        if source == target:
            return v
        blocks = [self.place(source, self.rel(target, p)) for p in range(self.chips)]
        runs = []
        for b in blocks:
            if runs and runs[-1][1] == b:
                runs[-1][1] = b + 1
            else:
                runs.append([b, b + 1])
        return jnp.concatenate(
            [v[:, a * self.block : e * self.block] for a, e in runs], axis=1
        )

    def split_columns(self, shards):
        sends, keeps = [], []
        for shard in shards:
            middle = shard.shape[1] // 2
            left, right = shard[:, :middle], shard[:, middle:]
            sends.append(self.pick(right, left))
            keeps.append(self.pick(left, right))
        got = self.other_core(jnp.concatenate(sends, axis=1))
        blocks, at = [], 0
        for keep in keeps:
            other = got[:, at : at + keep.shape[1]]
            at += keep.shape[1]
            blocks.append(
                self.pick(
                    jnp.concatenate([keep, other], axis=0), jnp.concatenate([other, keep], axis=0)
                )
            )
        return blocks

    def gather(self, block, order):
        held = block
        for bit in order[:0:-1]:
            held = jnp.concatenate([held, self.cross(held, bit)], axis=0)
        return held, self.cross(held, order[0])

    def gather_vector(self, shards):
        other = self.other_core(shards)
        held = self.pick(
            jnp.concatenate([shards, other], axis=1), jnp.concatenate([other, shards], axis=1)
        )
        return held

    def scatter(self, rows_space, columns, order):
        middle = self.width // 2
        send = dot_tn(rows_space[:, middle:], columns).astype(bf16)
        got = self.cross(send, order[0])
        total = dot_tn(rows_space[:, :middle], columns) + got.astype(f32)
        for bit in order[1:]:
            low, high = halves(total)
            total = low + self.cross(high.astype(bf16), bit).astype(f32)
        return total

    def scatter_vector(self, v, order):
        total = v
        for bit in order:
            middle = total.shape[1] // 2
            total = total[:, :middle] + self.cross(total[:, middle:], bit)
        return total

    def join_columns(self, total):
        low, high = halves(total)
        keep = self.pick(low, high)
        other = self.other_core(self.pick(high, low))
        return keep, other

    def side_by_side(self, keep, other):
        return self.pick(
            jnp.concatenate([keep, other], axis=1), jnp.concatenate([other, keep], axis=1)
        )


def times(h, weight):
    middle = h.shape[1] // 2
    return dot_nn(h[:, :middle], weight[0]) + dot_nn(h[:, middle:], weight[1])


def times_t(d, weight):
    return jnp.concatenate([dot_nt(d, weight[0]), dot_nt(d, weight[1])], axis=1)


def make_body(chips):
    def body(
        tokens,
        segment_ids,
        piece_starts,
        kv_cotangent,
        out_cotangent,
        attn_gain,
        w_query,
        w_key,
        w_value,
        output_weight,
        ffn_gain,
        w_gate,
        w_up,
        w_down,
    ):
        own_rows = tokens.shape[1]
        model_w = tokens.shape[2]
        head_w = w_key.shape[1]
        heads_n = model_w // head_w // 2
        all_rows = 2 * own_rows
        score_scale = head_w ** (-0.5)
        cube = Cube(chips, model_w)
        core = cube.core
        main = cube.order((0, 1, 2, 3))
        o_gate = main
        o_up = cube.order((1, 0, 2, 3))
        o_down = cube.order((0, 2, 3, 1))
        o_out = cube.order((1, 2, 3, 0))
        o_qkv = cube.order((1, 2, 3, 0))

        gains_own = cube.gather_vector(
            jnp.stack([attn_gain, ffn_gain], axis=0).astype(bf16)
        )
        wq_b, wkv_b, wo_b = cube.split_columns(
            [w_query, jnp.concatenate([w_key, w_value], axis=1), output_weight]
        )
        wqkv_b = jnp.concatenate([wq_b, wkv_b], axis=1)
        wg_b, wu_b, wd_b = cube.split_columns([w_gate, w_up, w_down])

        held = gains_own
        for bit in main[::-1]:
            held = jnp.concatenate([held, cube.cross(held, bit)], axis=1)
        gains = held.astype(f32)
        gain_one, gain_two = gains[0:1], gains[1:2]

        wqkv = cube.gather(wqkv_b, o_qkv)
        wo = cube.gather(wo_b, o_out)
        wg = cube.gather(wg_b, o_gate)
        wu = cube.gather(wu_b, o_up)
        wd = cube.gather(wd_b, o_down)

        tok_own = cube.to_space(tokens.reshape(own_rows, model_w), main)
        cot_own = cube.to_space(out_cotangent.reshape(own_rows, model_w), main)
        tok_all = jnp.concatenate([tok_own, cube.other_core(tok_own)], axis=0)
        cot_all = jnp.concatenate([cot_own, cube.other_core(cot_own)], axis=0)
        kvcot = kv_cotangent.reshape(own_rows, 2 * head_w)
        kvcot_k, kvcot_v = kvcot[:, :head_w], kvcot[:, head_w:]
        kvcot_mine = jnp.concatenate(
            [cube.pick(kvcot_k, kvcot_v), cube.other_core(cube.pick(kvcot_v, kvcot_k))], axis=0
        ).astype(f32)

        span = jnp.arange(own_rows, dtype=jnp.int32)
        positions = jnp.concatenate([core * own_rows + span, (1 - core) * own_rows + span])
        seg_low, seg_high = segment_ids[0, :own_rows], segment_ids[0, own_rows:]
        segs = cube.pick(
            jnp.concatenate([seg_low, seg_high]), jnp.concatenate([seg_high, seg_low])
        )
        start_val = piece_starts[0]
        inside = (positions >= start_val) & (positions < start_val + PIECE)
        visible = (segs[:, None] == segs[None, :]) & (
            (positions[None, :] <= positions[:, None]) | (inside[:, None] & inside[None, :])
        )
        cosine, sine_tab = rope_tables(positions, head_w)

        tok_f = tok_all.astype(f32)
        rms_one = rms_scale(tok_f)
        hidden = (tok_f * rms_one[:, None] * gain_one).astype(bf16)
        hidden_q = cube.respace(hidden, main, o_qkv)
        qkv = times(hidden_q, wqkv)
        q_cols = heads_n * head_w
        query_heads = (
            rotate(
                qkv[:, :q_cols].reshape(all_rows, heads_n, head_w),
                cosine[:, None, :],
                sine_tab[:, None, :],
            )
            * score_scale
        ).astype(bf16)
        kv_pre = qkv[:, q_cols:]
        kv_mine = cube.pick(rotate(kv_pre, cosine, sine_tab), kv_pre).astype(bf16)
        kv_other = swap_rows(cube.other_core(kv_mine))
        keys = cube.pick(kv_mine, kv_other)
        values = cube.pick(kv_other, kv_mine)
        scores = jnp.einsum("qhd,kd->hqk", query_heads, keys, preferred_element_type=f32)
        scores = jnp.where(visible[None], scores, masked_score)
        peak = jnp.max(scores, axis=-1, keepdims=True)
        expo = jnp.exp(scores - peak)
        totals = jnp.sum(expo, axis=-1, keepdims=True)
        log_total = peak + jnp.log(totals)
        probs_b = (expo / totals).astype(bf16)
        mixed = jnp.einsum("hqk,kd->qhd", probs_b, values, preferred_element_type=f32)
        mixed = mixed.reshape(all_rows, q_cols).astype(bf16)
        branch = times_t(mixed, wo)
        keep, send = halves(branch)
        branch = cube.respace(keep + cube.other_core(send), o_out, main)
        residual = tok_own.astype(f32) + branch
        rms_two = rms_scale(residual)
        normed_two = residual * rms_two[:, None]
        hidden_two = (normed_two * gain_two).astype(bf16)
        hidden_two = jnp.concatenate([hidden_two, cube.other_core(hidden_two)], axis=0)
        hidden_two_up = cube.respace(hidden_two, main, o_up)
        gate = times(hidden_two, wg)
        up = times(hidden_two_up, wu)
        sig = jax.nn.sigmoid(gate)
        silu = gate * sig
        act = (silu * up).astype(bf16)
        ffn = times_t(act, wd)
        keep, send = halves(ffn)
        ffn = cube.respace(keep + cube.other_core(send), o_down, main)
        layer_output = cube.from_space((residual + ffn).astype(bf16), main)

        cot_down = cube.respace(cot_all, main, o_down)
        down_sum = cube.scatter(cot_down, act, o_down)
        dact = times(cot_down, wd)
        dup = (dact * silu).astype(bf16)
        dgate = (dact * up * sig * (1.0 + gate * (1.0 - sig))).astype(bf16)
        gate_sum = cube.scatter(hidden_two, dgate, o_gate)
        up_sum = cube.scatter(hidden_two_up, dup, o_up)
        dhidden = times_t(dgate, wg) + cube.respace(times_t(dup, wu), o_up, main)
        keep, send = halves(dhidden)
        dhidden_two = keep + cube.other_core(send.astype(bf16)).astype(f32)
        ffn_gain_part = jnp.sum(dhidden_two * normed_two, axis=0, keepdims=True)
        dresidual = cot_own.astype(f32) + norm_back(dhidden_two * gain_two, normed_two, rms_two)
        dbranch = dresidual.astype(bf16)
        dbranch = jnp.concatenate([dbranch, cube.other_core(dbranch)], axis=0)
        dbranch_o = cube.respace(dbranch, main, o_out)
        dmixed = times(dbranch_o, wo).astype(bf16).reshape(all_rows, heads_n, head_w)
        out_sum = cube.scatter(dbranch_o, mixed, o_out)

        scores = jnp.einsum("qhd,kd->hqk", query_heads, keys, preferred_element_type=f32)
        probs = jnp.where(visible[None], jnp.exp(scores - log_total), 0.0)
        probs_b = probs.astype(bf16)
        dprobs = jnp.einsum("qhd,kd->hqk", dmixed, values, preferred_element_type=f32)
        dscores = (probs * (dprobs - jnp.sum(probs * dprobs, axis=-1, keepdims=True))).astype(bf16)
        dquery = jnp.einsum("hqk,kd->qhd", dscores, keys, preferred_element_type=f32)
        dkey = jnp.einsum("hqk,qhd->kd", dscores, query_heads, preferred_element_type=f32)
        dvalue = jnp.einsum("hqk,qhd->kd", probs_b, dmixed, preferred_element_type=f32)
        dkv = (
            cube.pick(dkey, dvalue)
            + swap_rows(cube.other_core(cube.pick(dvalue, dkey)))
            + kvcot_mine
        )
        dkv = cube.pick(rotate(dkv, cosine, -sine_tab), dkv).astype(bf16)
        dquery = (
            rotate(dquery * score_scale, cosine[:, None, :], -sine_tab[:, None, :])
            .reshape(all_rows, q_cols)
            .astype(bf16)
        )
        dqkv = jnp.concatenate([dquery, dkv], axis=1)
        qkv_sum = cube.scatter(hidden_q, dqkv, o_qkv)
        dhidden = times_t(dqkv, wqkv)
        keep, send = halves(dhidden)
        dhidden_one = cube.respace(
            keep + cube.other_core(send.astype(bf16)).astype(f32), o_qkv, main
        )
        normed_one = tok_own.astype(f32) * rms_one[:own_rows, None]
        attn_gain_part = jnp.sum(dhidden_one * normed_one, axis=0, keepdims=True)
        input_grad = dresidual + norm_back(
            dhidden_one * gain_one, normed_one, rms_one[:own_rows]
        )
        input_grad = cube.from_space(input_grad.astype(bf16), main)

        gain_sum = cube.scatter_vector(
            jnp.concatenate([attn_gain_part, ffn_gain_part], axis=0), main
        )
        g_low, g_high = gain_sum[:, : cube.block // 2], gain_sum[:, cube.block // 2 :]
        gain_grads = cube.pick(g_low, g_high) + cube.other_core(cube.pick(g_high, g_low))

        down_grad = cube.side_by_side(*cube.join_columns(down_sum))
        gate_grad = cube.side_by_side(*cube.join_columns(gate_sum))
        up_grad = cube.side_by_side(*cube.join_columns(up_sum))
        w_out_grad = cube.side_by_side(*cube.join_columns(out_sum))
        keep, other = cube.join_columns(qkv_sum)
        query_grad = cube.side_by_side(keep[:, :q_cols], other[:, :q_cols])
        key_grad = cube.pick(keep[:, q_cols:], other[:, q_cols:])
        value_grad = cube.pick(other[:, q_cols:], keep[:, q_cols:])
        return (
            layer_output.reshape(1, own_rows, model_w),
            input_grad.reshape(1, own_rows, model_w),
            gain_grads[0],
            query_grad,
            key_grad,
            value_grad,
            w_out_grad,
            gain_grads[1],
            gate_grad,
            up_grad,
            down_grad,
        )

    return body


def solution(mesh):
    rows_of = P(("fsdp", "seq"), None)
    vector = P(("fsdp", "seq"))
    acts = P("fsdp", "seq", None)
    return jax.shard_map(
        make_body(mesh.shape["fsdp"]),
        mesh=mesh,
        in_specs=(
            acts,
            P("fsdp", None),
            P("fsdp"),
            acts,
            acts,
            vector,
            rows_of,
            rows_of,
            rows_of,
            rows_of,
            vector,
            rows_of,
            rows_of,
            rows_of,
        ),
        out_specs=(
            acts,
            acts,
            vector,
            rows_of,
            rows_of,
            rows_of,
            rows_of,
            vector,
            rows_of,
            rows_of,
            rows_of,
        ),
        check_vma=False,
    )
```

```python
import functools

import jax
import jax.numpy as jnp
from jax import lax
from jax.experimental import pallas as pl
from jax.experimental.pallas import tpu as pltpu
from jax.sharding import PartitionSpec as P

PIECE = 256

norm_epsilon = 1e-05
rope_base = 10000.0
masked_score = -1e30

bf16 = jnp.bfloat16
f32 = jnp.float32


GATHER_FIRST = (3, 2, 0, 4, 1)
REDUCE_FIRST = (2, 1, 0, 3, 4)
GATHER_WAITS = (
    (3, 2, 0), (3, 3, 0), (2, 2, 0), (2, 3, 0), (3, 0, 0), (0, 2, 0), (0, 3, 0), (3, 1, 0),
    (4, 1, 0), (4, 2, 0), (1, 1, 0), (1, 2, 0), (3, 2, 1), (3, 3, 1), (2, 0, 0), (2, 1, 0),
    (2, 2, 1), (2, 3, 1), (0, 0, 0), (0, 1, 0), (0, 2, 1), (0, 3, 1), (4, 0, 0), (4, 1, 1),
    (4, 2, 1), (4, 3, 0), (1, 0, 0), (1, 1, 1), (1, 3, 0), (3, 1, 1), (4, 2, 2), (1, 2, 1),
    (2, 1, 1), (1, 2, 2), (0, 1, 1), (3, 3, 2), (4, 3, 1), (1, 3, 1), (3, 2, 2), (2, 2, 2),
    (4, 3, 2), (0, 3, 2), (2, 3, 2), (1, 3, 2), (0, 2, 2), (3, 3, 3), (4, 3, 3), (2, 3, 3),
    (0, 3, 3), (1, 3, 3),
)
REDUCE_WAITS = (
    (1, 0, 2), (1, 0, 1), (1, 0, 0), (1, 1, 1), (2, 0, 2), (1, 1, 0), (2, 0, 1), (2, 1, 1),
    (3, 0, 2), (2, 0, 0), (3, 0, 1), (2, 1, 0), (3, 0, 0), (0, 0, 3), (2, 2, 0), (0, 0, 2),
    (3, 1, 1), (0, 0, 1), (0, 0, 0), (4, 0, 2), (1, 2, 0), (3, 1, 0), (4, 0, 1), (4, 1, 1),
    (4, 0, 0), (3, 2, 0), (4, 1, 0), (0, 1, 2), (0, 1, 1), (4, 2, 0), (0, 1, 0), (0, 2, 1),
    (0, 2, 0), (0, 3, 0),
)


def rope_tables(positions, breadth):
    halfway = breadth // 2
    ladder = jnp.arange(halfway, dtype=f32) * (2.0 / breadth)
    frequency = rope_base ** (-ladder)
    angles = positions.astype(f32)[:, None] * frequency[None, :]
    angles = jnp.concatenate([angles, angles], axis=1)
    return (jnp.cos(angles), jnp.sin(angles))


def rotate(vectors, cosine, sine_tab):
    halfway = vectors.shape[-1] // 2
    turned = jnp.concatenate([-vectors[..., halfway:], vectors[..., :halfway]], axis=-1)
    return vectors * cosine + turned * sine_tab


def rms_scale(value_rows):
    return lax.rsqrt(jnp.mean(value_rows * value_rows, axis=-1) + norm_epsilon)


def norm_back(dnormed, normed, scales):
    inner_sum = jnp.mean(dnormed * normed, axis=-1, keepdims=True)
    return scales[:, None] * (dnormed - normed * inner_sum)


def dot_nn(a, b):
    return lax.dot_general(a, b, (((1,), (0,)), ((), ())), preferred_element_type=f32)


def dot_nt(a, b):
    return lax.dot_general(a, b, (((1,), (1,)), ((), ())), preferred_element_type=f32)


def dot_tn(a, b):
    return lax.dot_general(a, b, (((0,), (0,)), ((), ())), preferred_element_type=f32)


def halves(v):
    middle = v.shape[0] // 2
    return v[:middle], v[middle:]


def swap_rows(v):
    low, high = halves(v)
    return jnp.concatenate([high, low], axis=0)


class Cube:
    def __init__(self, chips, width):
        self.chips = chips
        self.bits = chips.bit_length() - 1
        self.width = width
        self.block = width // chips
        self.mine = lax.axis_index("fsdp")
        self.core = lax.axis_index("seq")

    def order(self, first):
        return tuple(b for b in first if b < self.bits) + tuple(
            b for b in range(self.bits) if b not in first
        )

    def rel(self, order, position):
        return sum(((position >> (self.bits - 1 - i)) & 1) << b for i, b in enumerate(order))

    def place(self, order, rel):
        return sum(((rel >> b) & 1) << (self.bits - 1 - i) for i, b in enumerate(order))

    def cross(self, v, bit):
        return lax.ppermute(v, "fsdp", [(i, i ^ (1 << bit)) for i in range(self.chips)])

    def other_core(self, v):
        return lax.ppermute(v, "seq", [(0, 1), (1, 0)])

    def pick(self, if_zero, if_one):
        return jnp.where(self.core == 0, if_zero, if_one)

    def to_space(self, v, order):
        starts = [(self.rel(order, p) ^ self.mine) * self.block for p in range(self.chips)]
        return jnp.concatenate(
            [lax.dynamic_slice_in_dim(v, s, self.block, axis=1) for s in starts], axis=1
        )

    def from_space(self, v, order):
        starts = [self.place(order, j ^ self.mine) * self.block for j in range(self.chips)]
        return jnp.concatenate(
            [lax.dynamic_slice_in_dim(v, s, self.block, axis=1) for s in starts], axis=1
        )

    def respace(self, v, source, target):
        if source == target:
            return v
        blocks = [self.place(source, self.rel(target, p)) for p in range(self.chips)]
        runs = []
        for b in blocks:
            if runs and runs[-1][1] == b:
                runs[-1][1] = b + 1
            else:
                runs.append([b, b + 1])
        return jnp.concatenate(
            [v[:, a * self.block : e * self.block] for a, e in runs], axis=1
        )

    def gather_vector(self, shards):
        other = self.other_core(shards)
        held = self.pick(
            jnp.concatenate([shards, other], axis=1), jnp.concatenate([other, shards], axis=1)
        )
        return held

    def send_high(self, rows_space, columns):
        return dot_tn(rows_space[:, self.width // 2 :], columns).astype(bf16)

    def add_low(self, rows_space, columns, send, order):
        got = self.cross(send, order[0])
        return (dot_tn(rows_space[:, : self.width // 2], columns) + got.astype(f32)).astype(bf16)


def axis_of(bit):
    return min(bit, 2)


def arrival_order(flows, table, extra):
    at = {flow.key: i for i, flow in enumerate(flows)}
    main = [i for i, flow in enumerate(flows) if flow.key[0] != extra]
    if len(table) == len(main) and all(key in at for key in table):
        main = [at[key] for key in table]
    else:
        clock, done = {}, {}
        queue = list(main)
        while queue:
            best = None
            for i in queue:
                if any(d not in done for d in flows[i].needs):
                    continue
                ready = max([done[d] for d in flows[i].needs], default=0.0)
                start = max(ready, clock.get(axis_of(flows[i].bit), 0.0))
                if best is None or start < best[0]:
                    best = (start, i)
            start, i = best
            clock[axis_of(flows[i].bit)] = done[i] = start + flows[i].size * (
                2 if flows[i].bit > 2 else 1
            )
            queue.remove(i)
        main.sort(key=lambda i: done[i])
    tiny = [i for i, flow in enumerate(flows) if flow.key[0] == extra]
    steps = 1 + max(flows[i].key[1] for i in tiny)
    ranked = [((k + 0.5) / len(main), i) for k, i in enumerate(main)]
    ranked += [((flows[i].key[1] + 1) / steps, i) for i in tiny]
    return [i for _, i in sorted(ranked)]


class Flow:
    def __init__(self, key, bit, needs, size, begin, count, target):
        self.key, self.bit, self.needs, self.size = key, bit, needs, size
        self.begin, self.count, self.target = begin, count, target


def gather_flows(orders, columns):
    flows, at = [], {}
    for w, order in enumerate(orders):
        for j, bit in enumerate(order[::-1]):
            for q in range(j + 1):
                begin, count = (0, 1) if q == 0 else (1 << (q - 1), 1 << (q - 1))
                needs = [] if q == 0 else list(at[(w, q - 1)])
                at.setdefault((w, j), []).append(len(flows))
                flows.append(
                    Flow((w, j, q), bit, needs, count * columns[w], begin, count, begin + (1 << j))
                )
    return flows


def reduce_flows(orders, columns):
    flows, at = [], {}
    for w, order in enumerate(orders):
        for i, bit in enumerate(order):
            j = len(order) - 1 - i
            for q in range(j, -1, -1):
                begin, count = (0, 1) if q == 0 else (1 << (q - 1), 1 << (q - 1))
                needs = [at[(w, early, j + 1)] for early in range(i)]
                at[(w, i, q)] = len(flows)
                flows.append(
                    Flow((w, i, q), bit, needs, count * columns[w], begin + (1 << j), count, begin)
                )
    return flows


def chip_across(bit):
    mine = lax.axis_index("fsdp")
    step = 1 << bit
    return mine + step - 2 * step * lax.rem(lax.div(mine, step), 2)


def meet_partners(bits):
    core = lax.axis_index("seq")
    barrier = pltpu.get_barrier_semaphore()
    pl.semaphore_signal(barrier, inc=1, device_id={"seq": 1 - core})
    for bit in range(bits):
        pl.semaphore_signal(barrier, inc=1, device_id={"fsdp": chip_across(bit)})
    pl.semaphore_wait(barrier, bits + 1)


def gather_kernel(bits, flows, waits, first, parts, own, *refs):
    ins = len({p[0] for p in parts})
    count = len({p[2] for p in parts})
    shards, gains_ref = refs[:ins], refs[ins]
    arrays = refs[ins + 1 : ins + 2 + count]
    keep_sem, pair_send, pair_recv, send_sem, recv_sem = refs[ins + 2 + count :]
    core = lax.axis_index("seq")
    meet_partners(bits)
    rows = pl.ds(pl.multiple_of(core * own, own), own)
    keeps, pairs = {}, {}
    gains_keep = pltpu.make_async_copy(
        gains_ref, arrays[count].at[pl.ds(0, 8)], keep_sem.at[len(parts)]
    )
    gains_keep.start()
    for out in first:
        for i, (source, half, target_out, at) in enumerate(parts):
            if target_out != out:
                continue
            target = arrays[out].at[rows, pl.ds(at, half)]
            theirs = pl.ds(pl.multiple_of((1 - core) * half, 128), half)
            mine = pl.ds(pl.multiple_of(core * half, 128), half)
            pairs[i] = pltpu.make_async_remote_copy(
                src_ref=shards[source].at[:, theirs],
                dst_ref=target,
                send_sem=pair_send.at[i],
                recv_sem=pair_recv.at[i],
                device_id={"seq": 1 - core},
            )
            pairs[i].start()
            keeps[i] = pltpu.make_async_copy(shards[source].at[:, mine], target, keep_sem.at[i])
            keeps[i].start()
    copies = []
    for i, flow in enumerate(flows):
        block = 8 if flow.key[0] == count else 2 * own
        ref = arrays[flow.key[0]]
        copies.append(
            pltpu.make_async_remote_copy(
                src_ref=ref.at[pl.ds(flow.begin * block, flow.count * block)],
                dst_ref=ref.at[pl.ds(flow.target * block, flow.count * block)],
                send_sem=send_sem.at[i],
                recv_sem=recv_sem.at[i],
                device_id={"fsdp": chip_across(flow.bit)},
            )
        )
    started, arrived = set(), set()

    def launch(array):
        for i, flow in enumerate(flows):
            if flow.key[0] == array and i not in started and arrived.issuperset(flow.needs):
                copies[i].start()
                started.add(i)

    gains_keep.wait()
    launch(count)
    for out in first:
        for i, part in enumerate(parts):
            if part[2] == out:
                keeps[i].wait()
                pairs[i].wait_recv()
        launch(out)
    for i in waits:
        copies[i].wait_recv()
        arrived.add(i)
        launch(flows[i].key[0])
    for i in pairs:
        pairs[i].wait_send()
    for copy in copies:
        copy.wait_send()


def gather_weights(cube, shards, parts, orders, gains):
    own = shards[0].shape[0]
    count = len(orders) - 1
    columns = [sum(p[1] for p in parts if p[2] == out) for out in range(count)]
    flows = gather_flows(orders, columns + [1])
    waits = arrival_order(flows, GATHER_WAITS, count)
    anywhere = pl.BlockSpec(memory_space=pl.ANY)
    return pl.pallas_call(
        functools.partial(gather_kernel, cube.bits, flows, waits, GATHER_FIRST, parts, own),
        out_shape=[jax.ShapeDtypeStruct((cube.width, c), bf16) for c in columns]
        + [jax.ShapeDtypeStruct((8 * cube.chips, 128), f32)],
        in_specs=[pl.BlockSpec(memory_space=pltpu.VMEM)] * (len(shards) + 1),
        out_specs=[anywhere] * (count + 1),
        scratch_shapes=[
            pltpu.SemaphoreType.DMA((len(parts) + 1,)),
            pltpu.SemaphoreType.DMA((len(parts),)),
            pltpu.SemaphoreType.DMA((len(parts),)),
            pltpu.SemaphoreType.DMA((len(flows),)),
            pltpu.SemaphoreType.DMA((len(flows),)),
        ],
        compiler_params=pltpu.CompilerParams(collective_id=0, has_side_effects=True),
        name="gather_weights",
    )(*shards, gains)


def reduce_kernel(bits, flows, waits, first, lengths, blocks, parts, *refs):
    count = len(lengths)
    outs_n = len({p[3] for p in parts})
    refs = list(refs)

    def take(k):
        taken = refs[:k]
        del refs[:k]
        return taken

    terms, outs = take(count), take(outs_n + 1)
    sums, lands, finals = take(count), take(count), take(count)
    load_sem, keep_sem, pair_send, pair_recv, send_sem, recv_sem = refs
    core = lax.axis_index("seq")
    loads = []
    for w in range(count):
        low = pl.ds(0, blocks[w] << (lengths[w] - 1))
        loads.append(pltpu.make_async_copy(terms[w].at[low], sums[w], load_sem.at[w]))
    for w in first:
        loads[w].start()
    meet_partners(bits)

    def land_of(flow):
        w, i, _ = flow.key
        base = sum(1 << (lengths[w] - 1 - early) for early in range(i))
        return lands[w].at[pl.ds((base + flow.target) * blocks[w], flow.count * blocks[w])]

    copies = []
    for i, flow in enumerate(flows):
        w, step, _ = flow.key
        rows = pl.ds(flow.begin * blocks[w], flow.count * blocks[w])
        copies.append(
            pltpu.make_async_remote_copy(
                src_ref=terms[w].at[rows] if step == 0 else sums[w].at[rows],
                dst_ref=land_of(flow),
                send_sem=send_sem.at[i],
                recv_sem=recv_sem.at[i],
                device_id={"fsdp": chip_across(flow.bit)},
            )
        )
    started, arrived, loaded = set(), set(), set()
    left = [sum(1 for flow in flows if flow.key[0] == w) for w in range(count)]
    ends = []

    def launch(array):
        for i, flow in enumerate(flows):
            if flow.key[0] == array and i not in started and arrived.issuperset(flow.needs):
                copies[i].start()
                started.add(i)

    def add(flow, last):
        w = flow.key[0]
        got = land_of(flow)
        begin = flow.target * blocks[w]
        rows = min(16, blocks[w])
        into = finals[w] if last else sums[w]

        def step(k, carry):
            here = pl.ds(pl.multiple_of(k * rows, rows), rows)
            there = pl.ds(pl.multiple_of(begin + k * rows, rows), rows)
            total = sums[w][there, :].astype(f32) + got[here, :].astype(f32)
            into[there, :] = total.astype(into.dtype)
            return carry

        lax.fori_loop(0, flow.count * blocks[w] // rows, step, 0)

    def finish(w):
        if w == count - 1:
            keep = pltpu.make_async_copy(
                finals[w], outs[outs_n].at[pl.ds(0, 8)], keep_sem.at[len(parts)]
            )
            pair = pltpu.make_async_remote_copy(
                src_ref=finals[w],
                dst_ref=outs[outs_n].at[pl.ds(8, 8)],
                send_sem=pair_send.at[len(parts)],
                recv_sem=pair_recv.at[len(parts)],
                device_id={"seq": 1 - core},
            )
            keep.start()
            pair.start()
            ends.extend([keep, pair])
            return
        half = blocks[w] // 2
        mine = pl.ds(pl.multiple_of(core * half, half), half)
        theirs = pl.ds(pl.multiple_of((1 - core) * half, half), half)
        for i, (array, at, columns, out) in enumerate(parts):
            if array != w:
                continue
            target = outs[out].at[:, pl.ds(pl.multiple_of(core * columns, 128), columns)]
            keep = pltpu.make_async_copy(
                finals[w].at[mine, pl.ds(at, columns)], target, keep_sem.at[i]
            )
            pair = pltpu.make_async_remote_copy(
                src_ref=finals[w].at[theirs, pl.ds(at, columns)],
                dst_ref=target,
                send_sem=pair_send.at[i],
                recv_sem=pair_recv.at[i],
                device_id={"seq": 1 - core},
            )
            keep.start()
            pair.start()
            ends.extend([keep, pair])

    for w in first:
        launch(w)
    for i in waits:
        w, step, _ = flows[i].key
        copies[i].wait_recv()
        if w not in loaded:
            loads[w].wait()
            loaded.add(w)
        add(flows[i], step == lengths[w] - 1)
        arrived.add(i)
        launch(w)
        left[w] -= 1
        if left[w] == 0:
            finish(w)
    for end in ends:
        end.wait()
    for copy in copies:
        copy.wait_send()


def reduce_weights(cube, terms, orders, parts, gains):
    terms = list(terms) + [gains]
    count = len(terms)
    columns = [t.shape[1] for t in terms]
    lengths = [len(order) for order in orders]
    blocks = [t.shape[0] >> n for t, n in zip(terms, lengths)]
    flows = reduce_flows(orders, columns[:-1] + [1])
    waits = arrival_order(flows, REDUCE_WAITS, count - 1)
    first = (count - 1,) + REDUCE_FIRST
    outs = {}
    for array, _, width, out in parts:
        outs[out] = jax.ShapeDtypeStruct((blocks[array] // 2, 2 * width), f32)
    anywhere = pl.BlockSpec(memory_space=pl.ANY)
    scratch = [
        pltpu.VMEM((b << (n - 1), c), t.dtype)
        for b, n, c, t in zip(blocks, lengths, columns, terms)
    ]
    scratch += [
        pltpu.VMEM((b * ((1 << n) - 1), c), t.dtype)
        for b, n, c, t in zip(blocks, lengths, columns, terms)
    ]
    scratch += [pltpu.VMEM((b, c), f32) for b, c in zip(blocks, columns)]
    for size in (count, len(parts) + 1, len(parts) + 1, len(parts) + 1, len(flows), len(flows)):
        scratch.append(pltpu.SemaphoreType.DMA((size,)))
    return pl.pallas_call(
        functools.partial(reduce_kernel, cube.bits, flows, waits, first, lengths, blocks, parts),
        out_shape=[outs[out] for out in sorted(outs)] + [jax.ShapeDtypeStruct((16, 128), f32)],
        in_specs=[anywhere] * count,
        out_specs=[anywhere] * (len(outs) + 1),
        scratch_shapes=scratch,
        compiler_params=pltpu.CompilerParams(
            collective_id=1, has_side_effects=True, vmem_limit_bytes=60 * 1024 * 1024
        ),
        name="reduce_weights",
    )(*terms)


def times(h, weight):
    return dot_nn(h, weight)


def times_t(d, weight):
    return dot_nt(d, weight)


def make_body(chips):
    def body(
        tokens,
        segment_ids,
        piece_starts,
        kv_cotangent,
        out_cotangent,
        attn_gain,
        w_query,
        w_key,
        w_value,
        output_weight,
        ffn_gain,
        w_gate,
        w_up,
        w_down,
    ):
        own_rows = tokens.shape[1]
        model_w = tokens.shape[2]
        head_w = w_key.shape[1]
        heads_n = model_w // head_w // 2
        all_rows = 2 * own_rows
        score_scale = head_w ** (-0.5)
        cube = Cube(chips, model_w)
        core = cube.core
        main = cube.order((0, 1, 2, 3))
        o_gate = main
        o_up = cube.order((1, 0, 2, 3))
        o_down = cube.order((2, 0, 1, 3))
        o_out = cube.order((2, 0, 1, 3))
        o_qkv = cube.order((1, 0, 2, 3))
        r_out = cube.order((2, 0, 3, 1))

        gains_own = cube.gather_vector(jnp.stack([attn_gain, ffn_gain], axis=0).astype(f32))
        half_q, half_f = model_w // 2, w_gate.shape[1] // 2
        wqkv, wo, wg, wu, wd, gains = gather_weights(
            cube,
            [
                w_query,
                jnp.concatenate([w_key, w_value], axis=1),
                output_weight,
                w_gate,
                w_up,
                w_down,
            ],
            [
                (0, half_q, 0, 0),
                (1, head_w, 0, half_q),
                (2, half_q, 1, 0),
                (3, half_f, 2, 0),
                (4, half_f, 3, 0),
                (5, half_f, 4, 0),
            ],
            [o_qkv, o_out, o_gate, o_up, o_down, main],
            jnp.pad(gains_own, ((0, 6), (0, 128 - cube.block))),
        )
        gains = gains.reshape(chips, 8, 128)[:, :2, : cube.block]
        gain_one = gains[:, 0].reshape(1, model_w)
        gain_two = gains[:, 1].reshape(1, model_w)

        tok_own = cube.to_space(tokens.reshape(own_rows, model_w), main)
        cot_own = cube.to_space(out_cotangent.reshape(own_rows, model_w), main)
        tok_all = jnp.concatenate([tok_own, cube.other_core(tok_own)], axis=0)
        cot_all = jnp.concatenate([cot_own, cube.other_core(cot_own)], axis=0)
        kvcot = kv_cotangent.reshape(own_rows, 2 * head_w)
        kvcot_k, kvcot_v = kvcot[:, :head_w], kvcot[:, head_w:]
        kvcot_mine = jnp.concatenate(
            [cube.pick(kvcot_k, kvcot_v), cube.other_core(cube.pick(kvcot_v, kvcot_k))], axis=0
        ).astype(f32)

        span = jnp.arange(own_rows, dtype=jnp.int32)
        positions = jnp.concatenate([core * own_rows + span, (1 - core) * own_rows + span])
        seg_low, seg_high = segment_ids[0, :own_rows], segment_ids[0, own_rows:]
        segs = cube.pick(
            jnp.concatenate([seg_low, seg_high]), jnp.concatenate([seg_high, seg_low])
        )
        start_val = piece_starts[0]
        inside = (positions >= start_val) & (positions < start_val + PIECE)
        visible = (segs[:, None] == segs[None, :]) & (
            (positions[None, :] <= positions[:, None]) | (inside[:, None] & inside[None, :])
        )
        cosine, sine_tab = rope_tables(positions, head_w)

        tok_f = tok_all.astype(f32)
        rms_one = rms_scale(tok_f)
        hidden = (tok_f * rms_one[:, None] * gain_one).astype(bf16)
        hidden_q = cube.respace(hidden, main, o_qkv)
        qkv = times(hidden_q, wqkv)
        q_cols = heads_n * head_w
        query_heads = (
            rotate(
                qkv[:, :q_cols].reshape(all_rows, heads_n, head_w),
                cosine[:, None, :],
                sine_tab[:, None, :],
            )
            * score_scale
        ).astype(bf16)
        kv_pre = qkv[:, q_cols:]
        kv_mine = cube.pick(rotate(kv_pre, cosine, sine_tab), kv_pre).astype(bf16)
        kv_other = swap_rows(cube.other_core(kv_mine))
        keys = cube.pick(kv_mine, kv_other)
        values = cube.pick(kv_other, kv_mine)
        scores = jnp.einsum("qhd,kd->hqk", query_heads, keys, preferred_element_type=f32)
        scores = jnp.where(visible[None], scores, masked_score)
        peak = jnp.max(scores, axis=-1, keepdims=True)
        expo = jnp.exp(scores - peak)
        totals = jnp.sum(expo, axis=-1, keepdims=True)
        log_total = peak + jnp.log(totals)
        probs_b = (expo / totals).astype(bf16)
        mixed = jnp.einsum("hqk,kd->qhd", probs_b, values, preferred_element_type=f32)
        mixed = mixed.reshape(all_rows, q_cols).astype(bf16)
        branch = times_t(mixed, wo)
        keep, send = halves(branch)
        branch = cube.respace(keep + cube.other_core(send), o_out, main)
        residual = tok_own.astype(f32) + branch
        rms_two = rms_scale(residual)
        normed_two = residual * rms_two[:, None]
        hidden_two = (normed_two * gain_two).astype(bf16)
        hidden_two = jnp.concatenate([hidden_two, cube.other_core(hidden_two)], axis=0)
        hidden_two_up = cube.respace(hidden_two, main, o_up)
        gate = times(hidden_two, wg)
        up = times(hidden_two_up, wu)
        sig = jax.nn.sigmoid(gate)
        silu = gate * sig
        act = (silu * up).astype(bf16)
        ffn = times_t(act, wd)
        keep, send = halves(ffn)
        ffn = cube.respace(keep + cube.other_core(send), o_down, main)
        layer_output = cube.from_space((residual + ffn).astype(bf16), main)

        cot_down = cube.respace(cot_all, main, o_down)
        down_send = cube.send_high(cot_down, act)
        cot_after, _ = lax.optimization_barrier((cot_down, down_send))
        dact = times(cot_after, wd)
        dup = (dact * silu).astype(bf16)
        dgate = (dact * up * sig * (1.0 + gate * (1.0 - sig))).astype(bf16)
        gate_send = cube.send_high(hidden_two, dgate)
        up_send = cube.send_high(hidden_two_up, dup)
        dgate_after, dup_after, _, _ = lax.optimization_barrier((dgate, dup, gate_send, up_send))
        dhidden = times_t(dgate_after, wg) + cube.respace(times_t(dup_after, wu), o_up, main)
        keep, send = halves(dhidden)
        dhidden_two = keep + cube.other_core(send.astype(bf16)).astype(f32)
        ffn_gain_part = jnp.sum(dhidden_two * normed_two, axis=0, keepdims=True)
        dresidual = cot_own.astype(f32) + norm_back(dhidden_two * gain_two, normed_two, rms_two)
        dbranch = dresidual.astype(bf16)
        dbranch = jnp.concatenate([dbranch, cube.other_core(dbranch)], axis=0)
        dbranch_o = cube.respace(dbranch, main, o_out)
        dmixed = times(dbranch_o, wo).astype(bf16).reshape(all_rows, heads_n, head_w)
        dbranch_r = cube.respace(dbranch, main, r_out)
        out_send = cube.send_high(dbranch_r, mixed)

        scores = jnp.einsum("qhd,kd->hqk", query_heads, keys, preferred_element_type=f32)
        probs = jnp.where(visible[None], jnp.exp(scores - log_total), 0.0)
        probs_b = probs.astype(bf16)
        dprobs = jnp.einsum("qhd,kd->hqk", dmixed, values, preferred_element_type=f32)
        dscores = (probs * (dprobs - jnp.sum(probs * dprobs, axis=-1, keepdims=True))).astype(bf16)
        dquery = jnp.einsum("hqk,kd->qhd", dscores, keys, preferred_element_type=f32)
        dkey = jnp.einsum("hqk,qhd->kd", dscores, query_heads, preferred_element_type=f32)
        dvalue = jnp.einsum("hqk,qhd->kd", probs_b, dmixed, preferred_element_type=f32)
        dkv = (
            cube.pick(dkey, dvalue)
            + swap_rows(cube.other_core(cube.pick(dvalue, dkey)))
            + kvcot_mine
        )
        dkv = cube.pick(rotate(dkv, cosine, -sine_tab), dkv).astype(bf16)
        dquery = (
            rotate(dquery * score_scale, cosine[:, None, :], -sine_tab[:, None, :])
            .reshape(all_rows, q_cols)
            .astype(bf16)
        )
        dqkv = jnp.concatenate([dquery, dkv], axis=1)
        qkv_term = dot_tn(hidden_q, dqkv).astype(bf16)
        dhidden = times_t(dqkv, wqkv)
        keep, send = halves(dhidden)
        dhidden_one = cube.respace(
            keep + cube.other_core(send.astype(bf16)).astype(f32), o_qkv, main
        )
        normed_one = tok_own.astype(f32) * rms_one[:own_rows, None]
        attn_gain_part = jnp.sum(dhidden_one * normed_one, axis=0, keepdims=True)
        input_grad = dresidual + norm_back(
            dhidden_one * gain_one, normed_one, rms_one[:own_rows]
        )
        input_grad = cube.from_space(input_grad.astype(bf16), main)

        gain_parts = jnp.stack([attn_gain_part[0], ffn_gain_part[0]], axis=0)
        gain_parts = jnp.pad(
            gain_parts.reshape(2, chips, cube.block), ((0, 6), (0, 0), (0, 128 - cube.block))
        )
        query_grad, kv_grad, w_out_grad, gate_grad, up_grad, down_grad, gain_sum = reduce_weights(
            cube,
            [
                qkv_term,
                cube.add_low(dbranch_r, mixed, out_send, r_out),
                cube.add_low(hidden_two, dgate, gate_send, o_gate),
                cube.add_low(hidden_two_up, dup, up_send, o_up),
                cube.add_low(cot_down, act, down_send, o_down),
            ],
            [o_qkv, r_out[1:], o_gate[1:], o_up[1:], o_down[1:], main],
            [
                (0, 0, q_cols, 0),
                (0, q_cols, head_w, 1),
                (1, 0, q_cols, 2),
                (2, 0, half_f, 3),
                (3, 0, half_f, 4),
                (4, 0, half_f, 5),
            ],
            gain_parts.transpose(1, 0, 2).reshape(8 * chips, 128),
        )
        key_grad, value_grad = kv_grad[:, :head_w], kv_grad[:, head_w:]
        gain_sum = (gain_sum[:2] + gain_sum[8:10])[:, : cube.block]
        gain_grads = cube.pick(gain_sum[:, : cube.block // 2], gain_sum[:, cube.block // 2 :])
        return (
            layer_output.reshape(1, own_rows, model_w),
            input_grad.reshape(1, own_rows, model_w),
            gain_grads[0],
            query_grad,
            key_grad,
            value_grad,
            w_out_grad,
            gain_grads[1],
            gate_grad,
            up_grad,
            down_grad,
        )

    return body


def solution(mesh):
    rows_of = P(("fsdp", "seq"), None)
    vector = P(("fsdp", "seq"))
    acts = P("fsdp", "seq", None)
    return jax.shard_map(
        make_body(mesh.shape["fsdp"]),
        mesh=mesh,
        in_specs=(
            acts,
            P("fsdp", None),
            P("fsdp"),
            acts,
            acts,
            vector,
            rows_of,
            rows_of,
            rows_of,
            rows_of,
            vector,
            rows_of,
            rows_of,
            rows_of,
        ),
        out_specs=(
            acts,
            acts,
            vector,
            rows_of,
            rows_of,
            rows_of,
            rows_of,
            vector,
            rows_of,
            rows_of,
            rows_of,
        ),
        check_vma=False,
    )
```
